32 devices in a mesh: row: 8 (over z, x), col: 4 (over y, core).
Axes of the slice: x: 2, y: 2, z: 4, core: 2. Of those that a mesh axis runs over, the one named last changes fastest.
Arguments:
- a_values: bfloat16 [2048, 2048], P('row', 'col'), may hold values from -0.125 to 0.125
- a_present: int32 [8, 8], P('row', 'col'), may hold values from 0 to 1, as said below
- b_values: bfloat16 [2048, 2048], P('row', 'col'), may hold values from -6 to 6
- b_present: int32 [8, 8], P('row', 'col'), may hold values 0 or 1
- w_values: bfloat16 [2048, 2048], P('row', 'col'), may hold values from -6 to 6
- w_present: int32 [8, 8], P('row', 'col'), may hold values 0 or 1
Outputs:
- masked: bfloat16 [2048, 2048], P('row', 'col')
- slot: float32 [8, 8], P('row', 'col')
- total: float32 [], replicated
The draws below stay inside these ranges and needn't reach their ends.
Inputs may be any that keep to these rules, and one draw needn't show every extreme that they name: `a_present`: 1 where a tile of a_values is present, else 0; the share of present tiles differs strongly from tile row to tile row.
All inputs are finite; a program needn't handle non-finite values. No bound on the sum of `b_present` or of `w_present` on one device may be relied on, other than what follows from the above.
Results may differ from the reference program's by a relative error of at most 0.001.
Values may be sent and summed in bfloat16 or wider, within the bound.
A program may use at most 128 MiB of HBM per device.

```python
import math
import jax
import jax.numpy as jnp

TILE = 256
TR_DEV = 1
TC_DEV = 2
MT = 8
KT = 8
NT = 8
N_ROW = 8
N_COL = 4


def draw_a_present(key, part):
    level_key = jax.random.fold_in(key, 11)
    roll_key = jax.random.fold_in(key, 23)
    level = jax.random.randint(level_key, (MT, 1), 1, 17)
    roll = jax.random.randint(roll_key, (MT, KT), 0, 16)
    return (roll < level).astype(jnp.int32)


def touch_ends(entries, rng, smallest, largest):
    longest = entries.shape.index(max(entries.shape))
    spots = []
    for shift in (0, 1):
        where = [jax.random.randint(jax.random.fold_in(rng, axis), (), 0, length) for axis, length in enumerate(entries.shape)]
        where[longest] = (where[longest] + shift) % entries.shape[longest]
        spots.append(tuple(where))
    return entries.at[spots[0]].set(smallest).at[spots[1]].set(largest)


def steps_of(stream_key, shape, split, least, largest):
    level, own = 1.0, jax.random.fold_in(stream_key, 6)
    for dim, parts in split:
        draws = jnp.exp(jax.random.uniform(jax.random.fold_in(own, dim), (parts,), jnp.float32, least / len(split), largest / len(split)))
        level = level * jnp.repeat(draws, shape[dim] // parts).reshape([-1 if axis == dim else 1 for axis in range(len(shape))])
    return level


def normal_values(stream_key, shape, width, most, pieces=(), kind=jnp.bfloat16):
    gain = steps_of(stream_key, shape, pieces, -0.22, 0.18) if pieces else 1.0
    drawn = jax.random.normal(stream_key, shape, jnp.float32) * width * gain
    return jnp.minimum(jnp.maximum(drawn, -most), most).astype(kind)


def setup_inputs(seed: int = 0) -> dict:
    key_list = jax.random.split(jax.random.key(seed), 7)
    return {
        "a_values": normal_values(key_list[0], (MT * TILE, KT * TILE), (KT * TILE) ** -0.5, 0.125, ((0, 8), (1, 4))),
        "a_present": draw_a_present(jax.random.fold_in(key_list[6], 71), 0),
        "b_values": normal_values(key_list[2], (KT * TILE, NT * TILE), 1.0, 6.0, ((0, 8), (1, 4))),
        "b_present": touch_ends((jax.random.randint(key_list[3], (KT, NT), 0, 4) < 3).astype(jnp.int32), jax.random.fold_in(key_list[3], 1), 0, 1),
        "w_values": normal_values(key_list[4], (MT * TILE, NT * TILE), 1.0, 6.0, ((0, 8), (1, 4))),
        "w_present": touch_ends((jax.random.randint(key_list[5], (MT, NT), 0, 4) < 3).astype(jnp.int32), jax.random.fold_in(key_list[5], 1), 0, 1),
    }


def expand(values, present):
    tile_rows, tile_cols = present.shape
    tile_size = values.shape[0] // tile_rows
    blocked = values.reshape(tile_rows, tile_size, tile_cols, tile_size)
    masked_tiles = blocked * present.astype(values.dtype)[:, None, :, None]
    return masked_tiles.reshape(values.shape)

def reference(a_values, a_present, b_values, b_present, w_values, w_present):
    a_eff = expand(a_values, a_present)
    b_eff = expand(b_values, b_present)
    w_eff = expand(w_values, w_present)
    product = jnp.dot(a_eff, b_eff, preferred_element_type=jnp.float32)
    weighted = product * w_eff.astype(jnp.float32)
    masked = weighted.astype(jnp.bfloat16)
    tile_link = jnp.dot(a_present, b_present, preferred_element_type=jnp.int32)
    present = w_present * (tile_link > 0).astype(jnp.int32)
    ordered = present.reshape(N_ROW, TR_DEV, N_COL, TC_DEV).transpose(0, 2, 1, 3).reshape(-1)
    before = jnp.cumsum(ordered).astype(jnp.int32) - ordered
    slot_flat = jnp.where(ordered > 0, before, -1).astype(jnp.int32)
    slot = slot_flat.reshape(N_ROW, N_COL, TR_DEV, TC_DEV).transpose(0, 2, 1, 3).reshape(MT, NT)
    total = jnp.sum(weighted) / (TILE * math.sqrt(MT * NT))
    return (masked, slot.astype(jnp.float32), total)
```

```python
import functools
import math

import jax
import jax.numpy as jnp
from jax import lax
from jax.experimental import pallas as pl
from jax.experimental.pallas import tpu as pltpu
from jax.sharding import PartitionSpec as P

MESH = pl.DeviceIdType.MESH
PIECES = 4


class Gather:
    def __init__(self, axis, n, buf, send_sem, recv_sem, pieces, diverted):
        self.axis, self.buf = axis, buf
        self.send_sem, self.recv_sem = send_sem, recv_sem
        self.me = lax.axis_index(axis)
        self.length = n // 2
        self.place, self.side = self.me // 2, self.me % 2
        self.pieces = pieces
        self.height = buf.shape[1] // pieces
        self.diverted = tuple(range(pieces - pieces // 2, pieces)) if diverted else ()

    def copy(self, way, slot, h):
        target = (self.me + 2, self.me - 2, self.me + 1 - 2 * self.side)[way]
        part = self.buf.at[slot, pl.ds(h * self.height, self.height), :]
        return pltpu.make_async_remote_copy(
            src_ref=part,
            dst_ref=part,
            send_sem=self.send_sem.at[way, slot, h],
            recv_sem=self.recv_sem.at[slot, h],
            device_id={self.axis: target},
            device_id_type=MESH,
        )

    def can_up(self):
        return self.place < self.length - 1

    def can_down(self):
        return self.place > 0

    def when_all(self, *conds):
        return pl.when(functools.reduce(jnp.logical_and, conds))

    def run(self, action, way, slot, h, *conds):
        @self.when_all(*conds)
        def _():
            action(self.copy(way, slot, h))

    def own(self, action):
        for h in range(self.pieces):
            self.run(action, 0, self.me, h, self.can_up())
            self.run(action, 1, self.me, h, self.can_down())
            action(self.copy(2, self.me, h))

    def line(self, d, receive, action):
        last = self.length - 1
        for h in range(self.pieces):
            for way, source, onward, end in (
                (0, self.place - d, self.can_up, 0),
                (1, self.place + d, self.can_down, last),
            ):
                slot = 2 * source + self.side
                there = jnp.logical_and(source >= 0, source <= last)
                if receive:
                    self.run(lambda c: c.wait_recv(), 2, slot, h, there)
                self.run(action, way, slot, h, there, onward())
                if h in self.diverted:
                    self.run(action, 2, slot, h, there, source != end)
                else:
                    self.run(action, 2, slot, h, there)

    def divert(self, d, receive, action):
        last = self.length - 1
        for h in self.diverted:
            for way, source, at, onward in (
                (0, 0, d, self.can_up),
                (1, last, last - d, self.can_down),
            ):
                slot = 2 * source + 1 - self.side
                here = self.place == at
                if receive:
                    self.run(lambda c: c.wait_recv(), 2, slot, h, here)
                self.run(action, way, slot, h, here, onward())

    def across(self, d):
        last = self.length - 1
        for h in range(self.pieces):
            for step, end in ((-1, 0), (1, last)):
                source = self.place + step * d
                slot = 2 * source + 1 - self.side
                there = jnp.logical_and(source >= 0, source <= last)
                if step > 0:
                    there = jnp.logical_and(there, d > 0)
                if h in self.diverted:
                    there = jnp.logical_and(there, jnp.logical_and(source != 0, source != last))
                self.run(lambda c: c.wait_recv(), 2, slot, h, there)


def start(c):
    c.start()


def wait_send(c):
    c.wait_send()


def kernel(
    n_row, n_col, tr, ka, br, tc, tile, scale,
    a_hbm, b_hbm, w_hbm, ap_ref, bp_ref, wp_ref,
    masked_hbm, slot_ref, total_ref,
    abuf, bbuf, wbuf, acc, obuf, amask, bmask, gate, ex,
    local_sem, a_send, a_recv, b_send, b_recv, am_send, am_recv, bm_send, bm_recv, ex_send, ex_recv,
):
    row, col = lax.axis_index("row"), lax.axis_index("col")
    me = row * n_col + col
    everyone = n_row * n_col
    ga = Gather("col", n_col, abuf, a_send, a_recv, min(PIECES, 2), False)
    gb = Gather("row", n_row, bbuf, b_send, b_recv, PIECES, True)

    loads = [
        pltpu.make_async_copy(b_hbm, bbuf.at[row], local_sem.at[0]),
        pltpu.make_async_copy(a_hbm, abuf.at[col], local_sem.at[1]),
        pltpu.make_async_copy(w_hbm, wbuf, local_sem.at[2]),
    ]
    for load in loads:
        load.start()

    barrier = pltpu.get_barrier_semaphore()

    def greet(o, _):
        other = lax.rem(me + o, everyone)
        pl.semaphore_signal(
            barrier, inc=1, device_id=(other // n_col, lax.rem(other, n_col)), device_id_type=MESH
        )
        return 0

    lax.fori_loop(1, everyone, greet, 0)

    lane = lax.broadcasted_iota(jnp.int32, (1, 128), 1)

    def packed(ref, rows, cols):
        v = jnp.zeros((1, 128), jnp.int32)
        for i in range(rows):
            for j in range(cols):
                v = jnp.where(lane == i * cols + j, ref[i : i + 1, j : j + 1], v)
        return v

    amask[col] = packed(ap_ref, tr, ka)
    bmask[row] = packed(bp_ref, br, tc)
    acc[...] = jnp.zeros_like(acc)
    pl.semaphore_wait(barrier, everyone - 1)

    def mask_copy(axis, mine, buf, send, recv, o, n):
        other = lax.rem(mine + o, n)
        return pltpu.make_async_remote_copy(
            src_ref=buf.at[mine], dst_ref=buf.at[mine],
            send_sem=send.at[other], recv_sem=recv.at[mine],
            device_id={axis: other}, device_id_type=MESH,
        )

    def mask_arrival(axis, mine, buf, send, recv, o, n):
        other = lax.rem(mine + o, n)
        return pltpu.make_async_remote_copy(
            src_ref=buf.at[other], dst_ref=buf.at[other],
            send_sem=send.at[other], recv_sem=recv.at[other],
            device_id={axis: other}, device_id_type=MESH,
        )

    mask_sets = (
        ("col", col, amask, am_send, am_recv, n_col),
        ("row", row, bmask, bm_send, bm_recv, n_row),
    )

    def masks(make, action):
        for axis, mine, buf, send, recv, n in mask_sets:
            def one(o, _):
                action(make(axis, mine, buf, send, recv, o, n))
                return 0
            lax.fori_loop(1, n, one, 0)

    loads[0].wait()
    gb.own(start)
    loads[1].wait()
    ga.own(start)
    masks(mask_copy, start)
    loads[2].wait()

    def lane_row(v, j):
        return jnp.broadcast_to(v[:, j : j + 1], (1, tile))

    def prepare():
        masks(mask_arrival, lambda c: c.wait_recv())
        links = [jnp.zeros((1, tc * tile), jnp.int32) for _ in range(tr)]
        for k in range(ka * n_col):
            bv = bmask[k // br]
            brow = jnp.concatenate([lane_row(bv, (k % br) * tc + j) for j in range(tc)], axis=1)
            av = amask[k // ka]
            for i in range(tr):
                at = i * ka + k % ka
                g = av[:, at : at + 1] * brow
                gate[k * tr + i] = g.astype(jnp.float32)
                links[i] = links[i] + g
        for i in range(tr):
            wrow = jnp.concatenate(
                [jnp.broadcast_to(wp_ref[i : i + 1, j : j + 1], (1, tile)) for j in range(tc)], axis=1
            )
            gate[ka * n_col * tr + i] = wrow.astype(jnp.float32)
            gate[ka * n_col * tr + tr + i] = jnp.where(links[i] > 0, wrow, 0).astype(jnp.float32)
        def a_step(d, _):
            ga.line(d, True, start)
            return 0
        lax.fori_loop(1, n_col // 2, a_step, 0)
        def a_across(d, _):
            ga.across(d)
            return 0
        lax.fori_loop(0, n_col // 2, a_across, 0)

    def compute(slot):
        for bi in range(br):
            k = slot * br + bi
            dev = k // ka
            lanes = pl.ds(pl.multiple_of(lax.rem(k, ka) * tile, tile), tile)
            block = bbuf[slot, bi * tile : (bi + 1) * tile, :]
            for i in range(tr):
                rows = slice(i * tile, (i + 1) * tile)
                g = gate[k * tr + i].astype(jnp.bfloat16)
                acc[rows, :] += jnp.dot(
                    abuf[dev, rows, lanes], block * g, preferred_element_type=jnp.float32
                )

    half = gb.length

    def step(d, _):
        gb.line(d, True, start)

        @pl.when(d == 1)
        def _():
            gb.divert(0, True, start)
            prepare()

        gb.divert(d, True, start)

        def near(j, _):
            place = gb.place + jnp.where(j == 0, 0, jnp.where(j == 1, -d, d))
            there = jnp.logical_and(place >= 0, place < half)
            there = jnp.logical_and(there, jnp.logical_or(j > 0, d == 1))
            there = jnp.logical_and(there, jnp.logical_or(j == 0, d < half))

            @pl.when(there)
            def _():
                compute(2 * place + gb.side)
            return 0

        lax.fori_loop(0, 3, near, 0)
        gb.across(d - 1)

        def far(j, _):
            place = gb.place + jnp.where(j == 0, 1 - d, d - 1)
            there = jnp.logical_and(place >= 0, place < half)
            there = jnp.logical_and(there, jnp.logical_or(j == 0, d > 1))

            @pl.when(there)
            def _():
                compute(2 * place + 1 - gb.side)
            return 0

        lax.fori_loop(0, 2, far, 0)
        return 0

    lax.fori_loop(1, half + 1, step, 0)

    base = ka * n_col * tr
    part = jnp.zeros((1, tc * tile), jnp.float32)
    for i in range(tr):
        rows = slice(i * tile, (i + 1) * tile)
        weighted = acc[rows, :] * (wbuf[rows, :].astype(jnp.float32) * gate[base + i])
        obuf[rows, :] = weighted.astype(jnp.bfloat16)
        part = part + jnp.sum(weighted, axis=0, keepdims=True)
    local_sum = jnp.sum(part, axis=1, keepdims=True)
    count = jnp.zeros((1, 1), jnp.float32)
    for i in range(tr):
        for j in range(tc):
            count = count + gate[base + tr + i][:, j * tile : j * tile + 1]
    ex[me] = jnp.where(lane == 0, local_sum, jnp.where(lane == 1, count, 0.0))

    def ex_copy(o, mine):
        other = lax.rem(me + o, everyone)
        slot = me if mine else other
        return pltpu.make_async_remote_copy(
            src_ref=ex.at[slot], dst_ref=ex.at[slot],
            send_sem=ex_send.at[other], recv_sem=ex_recv.at[slot],
            device_id=(other // n_col, lax.rem(other, n_col)), device_id_type=MESH,
        )

    def ex_start(o, _):
        ex_copy(o, True).start()
        return 0

    def ex_wait(o, _):
        ex_copy(o, False).wait_recv()
        return 0

    def ex_done(o, _):
        ex_copy(o, True).wait_send()
        return 0

    lax.fori_loop(1, everyone, ex_start, 0)
    store = pltpu.make_async_copy(obuf, masked_hbm, local_sem.at[3])
    store.start()

    gb.own(wait_send)
    ga.own(wait_send)
    masks(mask_copy, wait_send)

    def drain_b(d, _):
        gb.line(d, False, wait_send)
        gb.divert(d, False, wait_send)
        return 0

    gb.divert(0, False, wait_send)
    lax.fori_loop(1, half + 1, drain_b, 0)

    def drain_a(d, _):
        ga.line(d, False, wait_send)
        return 0

    lax.fori_loop(1, n_col // 2, drain_a, 0)

    lax.fori_loop(1, everyone, ex_wait, 0)
    sums, first = jnp.zeros((1, 128), jnp.float32), jnp.zeros((1, 128), jnp.float32)
    everything = ex[...]
    order = lax.broadcasted_iota(jnp.int32, (everyone, 1, 128), 0)
    sums = jnp.sum(everything, axis=0)
    first = jnp.sum(jnp.where(order < me, everything, 0.0), axis=0)
    total_ref[...] = sums[:, 0:1] / scale
    before = first[:, 1:2]
    for i in range(tr):
        for j in range(tc):
            there = gate[base + tr + i][:, j * tile : j * tile + 1]
            slot_ref[i : i + 1, j : j + 1] = jnp.where(there > 0, before, -1.0)
            before = before + there
    lax.fori_loop(1, everyone, ex_done, 0)
    store.wait()


def on_device(a_values, a_present, b_values, b_present, w_values, w_present):
    n_row, n_col = lax.axis_size("row"), lax.axis_size("col")
    tr, ka = a_present.shape
    br, tc = b_present.shape
    tile = a_values.shape[0] // tr
    kt = ka * n_col
    scale = tile * math.sqrt(tr * n_row * tc * n_col)
    everyone = n_row * n_col
    dma = pltpu.SemaphoreType.DMA
    hbm = pl.BlockSpec(memory_space=pl.ANY)
    vmem = pl.BlockSpec(memory_space=pltpu.VMEM)
    masked, slot, total = pl.pallas_call(
        functools.partial(kernel, n_row, n_col, tr, ka, br, tc, tile, scale),
        out_shape=(
            jax.ShapeDtypeStruct(w_values.shape, jnp.bfloat16),
            jax.ShapeDtypeStruct((tr, tc), jnp.float32),
            jax.ShapeDtypeStruct((1, 1), jnp.float32),
        ),
        in_specs=[hbm, hbm, hbm, vmem, vmem, vmem],
        out_specs=(hbm, vmem, vmem),
        scratch_shapes=[
            pltpu.VMEM((n_col, *a_values.shape), jnp.bfloat16),
            pltpu.VMEM((n_row, *b_values.shape), jnp.bfloat16),
            pltpu.VMEM(w_values.shape, jnp.bfloat16),
            pltpu.VMEM(w_values.shape, jnp.float32),
            pltpu.VMEM(w_values.shape, jnp.bfloat16),
            pltpu.VMEM((n_col, 1, 128), jnp.int32),
            pltpu.VMEM((n_row, 1, 128), jnp.int32),
            pltpu.VMEM((kt * tr + 2 * tr, 1, tc * tile), jnp.float32),
            pltpu.VMEM((everyone, 1, 128), jnp.float32),
            dma((4,)),
            dma((3, n_col, PIECES)),
            dma((n_col, PIECES)),
            dma((3, n_row, PIECES)),
            dma((n_row, PIECES)),
            dma((n_col,)),
            dma((n_col,)),
            dma((n_row,)),
            dma((n_row,)),
            dma((everyone,)),
            dma((everyone,)),
        ],
        compiler_params=pltpu.CompilerParams(
            collective_id=0, has_side_effects=True, vmem_limit_bytes=56 * 1024 * 1024
        ),
    )(a_values, b_values, w_values, a_present, b_present, w_present)
    return masked, slot, total.reshape(())


def solution(mesh):
    spec = P("row", "col")
    return jax.shard_map(
        on_device, mesh=mesh, in_specs=(spec,) * 6, out_specs=(spec, spec, P()), check_vma=False
    )
```

```python
import functools
import math

import jax
import jax.numpy as jnp
from jax import lax
from jax.experimental import pallas as pl
from jax.experimental.pallas import tpu as pltpu
from jax.sharding import PartitionSpec as P

MESH = pl.DeviceIdType.MESH
PIECES = 2
A_PIECES = 2


class Gather:
    def __init__(self, axis, n, buf, send_sem, recv_sem, pieces, diverted):
        self.axis, self.buf = axis, buf
        self.send_sem, self.recv_sem = send_sem, recv_sem
        self.me = lax.axis_index(axis)
        self.length = n // 2
        self.place, self.side = self.me // 2, self.me % 2
        self.pieces = pieces
        self.height = buf.shape[1] // pieces
        self.diverted = tuple(range(pieces - pieces // 2, pieces)) if diverted else ()

    def copy(self, way, slot, h):
        target = (self.me + 2, self.me - 2, self.me + 1 - 2 * self.side)[way]
        part = self.buf.at[slot, pl.ds(h * self.height, self.height), :]
        return pltpu.make_async_remote_copy(
            src_ref=part,
            dst_ref=part,
            send_sem=self.send_sem.at[way, slot, h],
            recv_sem=self.recv_sem.at[slot, h],
            device_id={self.axis: target},
            device_id_type=MESH,
        )

    def can_up(self):
        return self.place < self.length - 1

    def can_down(self):
        return self.place > 0

    def when_all(self, *conds):
        return pl.when(functools.reduce(jnp.logical_and, conds))

    def run(self, action, way, slot, h, *conds):
        @self.when_all(*conds)
        def _():
            action(self.copy(way, slot, h))

    def own(self, action):
        for h in range(self.pieces):
            self.run(action, 0, self.me, h, self.can_up())
            self.run(action, 1, self.me, h, self.can_down())
            action(self.copy(2, self.me, h))

    def line(self, d, receive, action):
        last = self.length - 1
        for h in range(self.pieces):
            for way, source, onward, end in (
                (0, self.place - d, self.can_up, 0),
                (1, self.place + d, self.can_down, last),
            ):
                slot = 2 * source + self.side
                there = jnp.logical_and(source >= 0, source <= last)
                if receive:
                    self.run(lambda c: c.wait_recv(), 2, slot, h, there)
                self.run(action, way, slot, h, there, onward())
                if h in self.diverted:
                    self.run(action, 2, slot, h, there, source != end)
                else:
                    self.run(action, 2, slot, h, there)

    def divert(self, d, receive, action):
        last = self.length - 1
        for h in self.diverted:
            for way, source, at, onward in (
                (0, 0, d, self.can_up),
                (1, last, last - d, self.can_down),
            ):
                slot = 2 * source + 1 - self.side
                here = self.place == at
                if receive:
                    self.run(lambda c: c.wait_recv(), 2, slot, h, here)
                self.run(action, way, slot, h, here, onward())

    def across(self, d):
        last = self.length - 1
        for h in range(self.pieces):
            for step, end in ((-1, 0), (1, last)):
                source = self.place + step * d
                slot = 2 * source + 1 - self.side
                there = jnp.logical_and(source >= 0, source <= last)
                if step > 0:
                    there = jnp.logical_and(there, d > 0)
                if h in self.diverted:
                    there = jnp.logical_and(there, jnp.logical_and(source != 0, source != last))
                self.run(lambda c: c.wait_recv(), 2, slot, h, there)


def start(c):
    c.start()


def wait_send(c):
    c.wait_send()


def kernel(
    n_row, n_col, tr, ka, br, tc, tile, scale,
    a_hbm, b_hbm, w_hbm, ap_hbm, bp_hbm, wp_hbm,
    obuf, slot_ref, total_ref,
    abuf, bbuf, wbuf, acc, ap_ref, bp_ref, wp_ref, amask, bmask, ex,
    local_sem, a_send, a_recv, b_send, b_recv, am_send, am_recv, bm_send, bm_recv, ex_send, ex_recv, token,
):
    row, col = lax.axis_index("row"), lax.axis_index("col")
    me = row * n_col + col
    everyone = n_row * n_col
    ga = Gather("col", n_col, abuf, a_send, a_recv, A_PIECES, False)
    gb = Gather("row", n_row, bbuf, b_send, b_recv, PIECES, True)

    pairs = (
        (bp_hbm, bp_ref), (b_hbm, bbuf.at[row]), (ap_hbm, ap_ref),
        (a_hbm, abuf.at[col]), (wp_hbm, wp_ref), (w_hbm, wbuf),
    )
    loads = [pltpu.make_async_copy(x, y, local_sem.at[i]) for i, (x, y) in enumerate(pairs)]
    for load in loads:
        load.start()

    def signal(sem, g, shift):
        pl.semaphore_signal(sem, inc=1, device_id={g.axis: g.me + shift}, device_id_type=MESH)

    barrier = pltpu.get_barrier_semaphore()
    greeted = 0
    for g in (gb, ga):
        signal(barrier, g, 1 - 2 * g.side)
        pl.when(g.can_up())(functools.partial(signal, barrier, g, 2))
        pl.when(g.can_down())(functools.partial(signal, barrier, g, -2))
        greeted += 1 + g.can_up().astype(jnp.int32) + g.can_down().astype(jnp.int32)

    def gated(get, put, present, rows, cols):
        for i in range(rows):
            for j in range(cols):
                m = present[i : i + 1, j : j + 1].astype(jnp.float32).astype(jnp.bfloat16)
                put(i, j, get(i, j) * m)

    def gate_block(buf, slot, present, rows, cols):
        def part(i, j):
            return (slot, slice(i * tile, (i + 1) * tile), slice(j * tile, (j + 1) * tile))

        def put(i, j, v):
            buf[part(i, j)] = v

        gated(lambda i, j: buf[part(i, j)], put, present, rows, cols)

    loads[0].wait()
    loads[1].wait()
    gate_block(bbuf, row, bp_ref, br, tc)
    loads[2].wait()
    loads[3].wait()
    gate_block(abuf, col, ap_ref, tr, ka)
    pl.semaphore_wait(barrier, greeted)
    gb.own(start)
    ga.own(start)

    for i, g in enumerate((ga, gb)):
        pair, up, down = token.at[3 * i], token.at[3 * i + 1], token.at[3 * i + 2]
        signal(pair, g, 1 - 2 * g.side)
        if i == 0:
            lane = lax.broadcasted_iota(jnp.int32, (1, 128), 1)

            def packed(ref, rows, cols):
                v = jnp.zeros((1, 128), jnp.int32)
                for r in range(rows):
                    for c in range(cols):
                        v = jnp.where(lane == r * cols + c, ref[r : r + 1, c : c + 1], v)
                return v

            amask[col] = packed(ap_ref, tr, ka)
            bmask[row] = packed(bp_ref, br, tc)
        pl.semaphore_wait(pair, 1)
        last = g.length - 1
        first_up = jnp.logical_and(g.place == 0, g.can_up())
        first_down = jnp.logical_and(g.place == last, g.can_down())
        pl.when(first_up)(functools.partial(signal, up, g, 2))
        pl.when(first_down)(functools.partial(signal, down, g, -2))
        if i == 0:
            acc[...] = jnp.zeros_like(acc)

        @pl.when(g.can_down())
        def _():
            pl.semaphore_wait(up, 1)
            pl.when(g.can_up())(functools.partial(signal, up, g, 2))

        @pl.when(g.can_up())
        def _():
            pl.semaphore_wait(down, 1)
            pl.when(g.can_down())(functools.partial(signal, down, g, -2))

    mask_sets = (
        ("col", col, amask, am_send, am_recv, n_col),
        ("row", row, bmask, bm_send, bm_recv, n_row),
    )

    def masks(arriving, action):
        for axis, mine, buf, send, recv, n in mask_sets:
            def one(o, _):
                other = lax.rem(mine + o, n)
                slot = other if arriving else mine
                action(pltpu.make_async_remote_copy(
                    src_ref=buf.at[slot], dst_ref=buf.at[slot],
                    send_sem=send.at[other], recv_sem=recv.at[slot],
                    device_id={axis: other}, device_id_type=MESH,
                ))
                return 0
            lax.fori_loop(1, n, one, 0)

    masks(False, start)
    loads[4].wait()
    loads[5].wait()
    for i in range(tr):
        for j in range(tc):
            at = (slice(i * tile, (i + 1) * tile), slice(j * tile, (j + 1) * tile))
            m = wp_ref[i : i + 1, j : j + 1].astype(jnp.float32).astype(jnp.bfloat16)
            wbuf[at] = wbuf[at] * m

    def gather_a():
        def a_step(d, _):
            ga.line(d, True, start)
            return 0

        def a_across(d, _):
            ga.across(d)
            return 0

        lax.fori_loop(1, ga.length, a_step, 0)
        lax.fori_loop(0, ga.length, a_across, 0)

    def compute(slot):
        for bi in range(br):
            k = slot * br + bi
            dev = k // ka
            lanes = pl.ds(pl.multiple_of(lax.rem(k, ka) * tile, tile), tile)
            block = bbuf[slot, bi * tile : (bi + 1) * tile, :]
            for i in range(tr):
                rows = slice(i * tile, (i + 1) * tile)
                acc[rows, :] += jnp.dot(
                    abuf[dev, rows, lanes], block, preferred_element_type=jnp.float32
                )

    half = gb.length

    def step(d, _):
        gb.line(d, True, start)

        @pl.when(d == 1)
        def _():
            gb.divert(0, True, start)
            gather_a()

        gb.divert(d, True, start)

        def near(j, _):
            place = gb.place + jnp.where(j == 0, 0, jnp.where(j == 1, -d, d))
            there = jnp.logical_and(place >= 0, place < half)
            there = jnp.logical_and(there, jnp.logical_or(j > 0, d == 1))
            there = jnp.logical_and(there, jnp.logical_or(j == 0, d < half))

            @pl.when(there)
            def _():
                compute(2 * place + gb.side)
            return 0

        lax.fori_loop(0, 3, near, 0)

        @pl.when(d == half)
        def _():
            masks(True, lambda c: c.wait_recv())

        gb.across(d - 1)

        def far(j, _):
            place = gb.place + jnp.where(j == 0, 1 - d, d - 1)
            there = jnp.logical_and(place >= 0, place < half)
            there = jnp.logical_and(there, jnp.logical_or(j == 0, d > 1))

            @pl.when(there)
            def _():
                compute(2 * place + 1 - gb.side)
            return 0

        lax.fori_loop(0, 2, far, 0)
        return 0

    lax.fori_loop(1, half + 1, step, 0)

    there = {}
    links = [[jnp.zeros((1, 128), jnp.int32) for _ in range(br)] for _ in range(tr)]
    for k in range(ka * n_col):
        for i in range(tr):
            at = i * ka + k % ka
            links[i][k % br] += amask[k // ka][:, at : at + 1] * bmask[k // br]
    for i in range(tr):
        for j in range(tc):
            link = sum(links[i][bi][:, bi * tc + j : bi * tc + j + 1] for bi in range(br))
            there[i, j] = jnp.where(link > 0, wp_ref[i : i + 1, j : j + 1], 0).astype(jnp.float32)
    count = sum(there.values())

    weighted = acc[...] * wbuf[...].astype(jnp.float32)
    obuf[...] = weighted.astype(jnp.bfloat16)
    part = jnp.sum(weighted, axis=0, keepdims=True)
    local_sum = jnp.sum(part, axis=1, keepdims=True)
    ex[me] = jnp.where(lane == 0, local_sum, jnp.where(lane == 1, count, 0.0))

    def ex_copy(o, mine):
        other = lax.rem(me + o, everyone)
        slot = me if mine else other
        return pltpu.make_async_remote_copy(
            src_ref=ex.at[slot], dst_ref=ex.at[slot],
            send_sem=ex_send.at[other], recv_sem=ex_recv.at[slot],
            device_id=(other // n_col, lax.rem(other, n_col)), device_id_type=MESH,
        )

    def ex_start(o, _):
        ex_copy(o, True).start()
        return 0

    def ex_wait(o, _):
        ex_copy(o, False).wait_recv()
        return 0

    def ex_done(o, _):
        ex_copy(o, True).wait_send()
        return 0

    lax.fori_loop(1, everyone, ex_start, 0)

    gb.own(wait_send)
    ga.own(wait_send)
    masks(False, wait_send)
    gb.divert(0, False, wait_send)

    def drain_b(d, _):
        gb.line(d, False, wait_send)
        gb.divert(d, False, wait_send)
        return 0

    def drain_a(d, _):
        ga.line(d, False, wait_send)
        return 0

    lax.fori_loop(1, half + 1, drain_b, 0)
    lax.fori_loop(1, ga.length, drain_a, 0)

    lax.fori_loop(1, everyone, ex_wait, 0)
    everything = ex[...]
    order = lax.broadcasted_iota(jnp.int32, (everyone, 1, 128), 0)
    sums = jnp.sum(everything, axis=0)
    first = jnp.sum(jnp.where(order < me, everything, 0.0), axis=0)
    total_ref[...] = sums[:, 0:1] / scale
    before = first[:, 1:2]
    for i in range(tr):
        for j in range(tc):
            slot_ref[i : i + 1, j : j + 1] = jnp.where(there[i, j] > 0, before, -1.0)
            before = before + there[i, j]
    lax.fori_loop(1, everyone, ex_done, 0)


def on_device(a_values, a_present, b_values, b_present, w_values, w_present):
    n_row, n_col = lax.axis_size("row"), lax.axis_size("col")
    tr, ka = a_present.shape
    br, tc = b_present.shape
    tile = a_values.shape[0] // tr
    scale = tile * math.sqrt(tr * n_row * tc * n_col)
    everyone = n_row * n_col
    dma = pltpu.SemaphoreType.DMA
    hbm = pl.BlockSpec(memory_space=pl.ANY)
    vmem = pl.BlockSpec(memory_space=pltpu.VMEM)
    masked, slot, total = pl.pallas_call(
        functools.partial(kernel, n_row, n_col, tr, ka, br, tc, tile, scale),
        out_shape=(
            jax.ShapeDtypeStruct(w_values.shape, jnp.bfloat16),
            jax.ShapeDtypeStruct((tr, tc), jnp.float32),
            jax.ShapeDtypeStruct((1, 1), jnp.float32),
        ),
        in_specs=[hbm] * 6,
        out_specs=(vmem, vmem, vmem),
        scratch_shapes=[
            pltpu.VMEM((n_col, *a_values.shape), jnp.bfloat16),
            pltpu.VMEM((n_row, *b_values.shape), jnp.bfloat16),
            pltpu.VMEM(w_values.shape, jnp.bfloat16),
            pltpu.VMEM(w_values.shape, jnp.float32),
            pltpu.VMEM(a_present.shape, jnp.int32),
            pltpu.VMEM(b_present.shape, jnp.int32),
            pltpu.VMEM(w_present.shape, jnp.int32),
            pltpu.VMEM((n_col, 1, 128), jnp.int32),
            pltpu.VMEM((n_row, 1, 128), jnp.int32),
            pltpu.VMEM((everyone, 1, 128), jnp.float32),
            dma((6,)),
            dma((3, n_col, A_PIECES)),
            dma((n_col, A_PIECES)),
            dma((3, n_row, PIECES)),
            dma((n_row, PIECES)),
            dma((n_col,)),
            dma((n_col,)),
            dma((n_row,)),
            dma((n_row,)),
            dma((everyone,)),
            dma((everyone,)),
            pltpu.SemaphoreType.REGULAR((6,)),
        ],
        compiler_params=pltpu.CompilerParams(
            collective_id=0, has_side_effects=True, vmem_limit_bytes=56 * 1024 * 1024
        ),
    )(a_values, b_values, w_values, a_present, b_present, w_present)
    return masked, slot, total.reshape(())


def solution(mesh):
    spec = P("row", "col")
    return jax.shard_map(
        on_device, mesh=mesh, in_specs=(spec,) * 6, out_specs=(spec, spec, P()), check_vma=False
    )
```

```python
import functools
import math

import jax
import jax.numpy as jnp
from jax import lax
from jax.experimental import pallas as pl
from jax.experimental.pallas import tpu as pltpu
from jax.sharding import PartitionSpec as P

MESH = pl.DeviceIdType.MESH
PIECES = 2
A_PIECES = 2


class Gather:
    def __init__(self, axis, n, buf, send_sem, recv_sem, pieces, diverted):
        self.axis, self.buf = axis, buf
        self.send_sem, self.recv_sem = send_sem, recv_sem
        self.me = lax.axis_index(axis)
        self.length = n // 2
        self.place, self.side = self.me // 2, self.me % 2
        self.pieces = pieces
        self.height = buf.shape[1] // pieces
        self.diverted = tuple(range(pieces - pieces // 2, pieces)) if diverted else ()

    def copy(self, way, slot, h):
        target = (self.me + 2, self.me - 2, self.me + 1 - 2 * self.side)[way]
        part = self.buf.at[slot, pl.ds(h * self.height, self.height), :]
        return pltpu.make_async_remote_copy(
            src_ref=part,
            dst_ref=part,
            send_sem=self.send_sem.at[way, slot, h],
            recv_sem=self.recv_sem.at[slot, h],
            device_id={self.axis: target},
            device_id_type=MESH,
        )

    def can_up(self):
        return self.place < self.length - 1

    def can_down(self):
        return self.place > 0

    def when_all(self, *conds):
        return pl.when(functools.reduce(jnp.logical_and, conds))

    def run(self, action, way, slot, h, *conds):
        @self.when_all(*conds)
        def _():
            action(self.copy(way, slot, h))

    def own(self, action):
        for h in range(self.pieces):
            self.run(action, 0, self.me, h, self.can_up())
            self.run(action, 1, self.me, h, self.can_down())
            action(self.copy(2, self.me, h))

    def line(self, d, receive, action):
        last = self.length - 1
        for h in range(self.pieces):
            for way, source, onward, end in (
                (0, self.place - d, self.can_up, 0),
                (1, self.place + d, self.can_down, last),
            ):
                slot = 2 * source + self.side
                there = jnp.logical_and(source >= 0, source <= last)
                if receive:
                    self.run(lambda c: c.wait_recv(), 2, slot, h, there)
                self.run(action, way, slot, h, there, onward())
                if h in self.diverted:
                    self.run(action, 2, slot, h, there, source != end)
                else:
                    self.run(action, 2, slot, h, there)

    def divert(self, d, receive, action):
        last = self.length - 1
        for h in self.diverted:
            for way, source, at, onward in (
                (0, 0, d, self.can_up),
                (1, last, last - d, self.can_down),
            ):
                slot = 2 * source + 1 - self.side
                here = self.place == at
                if receive:
                    self.run(lambda c: c.wait_recv(), 2, slot, h, here)
                self.run(action, way, slot, h, here, onward())

    def across(self, d):
        last = self.length - 1
        for h in range(self.pieces):
            for step, end in ((-1, 0), (1, last)):
                source = self.place + step * d
                slot = 2 * source + 1 - self.side
                there = jnp.logical_and(source >= 0, source <= last)
                if step > 0:
                    there = jnp.logical_and(there, d > 0)
                if h in self.diverted:
                    there = jnp.logical_and(there, jnp.logical_and(source != 0, source != last))
                self.run(lambda c: c.wait_recv(), 2, slot, h, there)


def start(c):
    c.start()


def wait_send(c):
    c.wait_send()


def kernel(
    n_row, n_col, tr, ka, br, tc, tile,
    a_hbm, b_hbm, w_hbm, ap_hbm, bp_hbm, wp_hbm,
    obuf, slot_ref, total_ref,
    abuf, bbuf, wbuf, acc, ap_ref, bp_ref, wp_ref, amask, bmask, ex,
    local_sem, a_send, a_recv, b_send, b_recv, am_send, am_recv, bm_send, bm_recv, ex_send, ex_recv, token,
):
    row, col = lax.axis_index("row"), lax.axis_index("col")
    me = row * n_col + col
    everyone = n_row * n_col
    ga = Gather("col", n_col, abuf, a_send, a_recv, A_PIECES, False)
    gb = Gather("row", n_row, bbuf, b_send, b_recv, PIECES, True)

    def signal(sem, g, shift):
        pl.semaphore_signal(sem, inc=1, device_id={g.axis: g.me + shift}, device_id_type=MESH)

    barrier = pltpu.get_barrier_semaphore()
    greeted = 0
    for g in (gb, ga):
        signal(barrier, g, 1 - 2 * g.side)
        pl.when(g.can_up())(functools.partial(signal, barrier, g, 2))
        pl.when(g.can_down())(functools.partial(signal, barrier, g, -2))
        greeted += 1 + g.can_up().astype(jnp.int32) + g.can_down().astype(jnp.int32)

    pairs = (
        (bp_hbm, bp_ref), (b_hbm, bbuf.at[row]), (ap_hbm, ap_ref),
        (a_hbm, abuf.at[col]), (wp_hbm, wp_ref), (w_hbm, wbuf),
    )
    loads = [pltpu.make_async_copy(x, y, local_sem.at[i]) for i, (x, y) in enumerate(pairs)]
    for load in loads:
        load.start()

    def gated(get, put, present, rows, cols):
        for i in range(rows):
            for j in range(cols):
                m = present[i : i + 1, j : j + 1].astype(jnp.float32).astype(jnp.bfloat16)
                put(i, j, get(i, j) * m)

    def gate_block(buf, slot, present, rows, cols):
        def part(i, j):
            return (slot, slice(i * tile, (i + 1) * tile), slice(j * tile, (j + 1) * tile))

        def put(i, j, v):
            buf[part(i, j)] = v

        gated(lambda i, j: buf[part(i, j)], put, present, rows, cols)

    loads[0].wait()
    loads[1].wait()
    gate_block(bbuf, row, bp_ref, br, tc)
    loads[2].wait()
    loads[3].wait()
    gate_block(abuf, col, ap_ref, tr, ka)
    pl.semaphore_wait(barrier, greeted)
    gb.own(start)
    ga.own(start)

    for i, g in enumerate((ga, gb)):
        pair, up, down = token.at[3 * i], token.at[3 * i + 1], token.at[3 * i + 2]
        signal(pair, g, 1 - 2 * g.side)
        if i == 0:
            lane = lax.broadcasted_iota(jnp.int32, (1, 128), 1)

            def packed(ref, rows, cols):
                v = jnp.zeros((1, 128), jnp.int32)
                for r in range(rows):
                    for c in range(cols):
                        v = jnp.where(lane == r * cols + c, ref[r : r + 1, c : c + 1], v)
                return v

            amask[col] = packed(ap_ref, tr, ka)
            bmask[row] = packed(bp_ref, br, tc)
        pl.semaphore_wait(pair, 1)
        last = g.length - 1
        first_up = jnp.logical_and(g.place == 0, g.can_up())
        first_down = jnp.logical_and(g.place == last, g.can_down())
        pl.when(first_up)(functools.partial(signal, up, g, 2))
        pl.when(first_down)(functools.partial(signal, down, g, -2))
        if i == 0:
            acc[...] = jnp.zeros_like(acc)

        @pl.when(g.can_down())
        def _():
            pl.semaphore_wait(up, 1)
            pl.when(g.can_up())(functools.partial(signal, up, g, 2))

        @pl.when(g.can_up())
        def _():
            pl.semaphore_wait(down, 1)
            pl.when(g.can_down())(functools.partial(signal, down, g, -2))

    mask_sets = (
        ("col", col, amask, am_send, am_recv, n_col),
        ("row", row, bmask, bm_send, bm_recv, n_row),
    )

    def masks(arriving, action):
        for axis, mine, buf, send, recv, n in mask_sets:
            def one(o, _):
                other = lax.rem(mine + o, n)
                slot = other if arriving else mine
                action(pltpu.make_async_remote_copy(
                    src_ref=buf.at[slot], dst_ref=buf.at[slot],
                    send_sem=send.at[other], recv_sem=recv.at[slot],
                    device_id={axis: other}, device_id_type=MESH,
                ))
                return 0
            lax.fori_loop(1, n, one, 0)

    masks(False, start)
    loads[4].wait()
    loads[5].wait()
    for i in range(tr):
        for j in range(tc):
            at = (slice(i * tile, (i + 1) * tile), slice(j * tile, (j + 1) * tile))
            m = wp_ref[i : i + 1, j : j + 1].astype(jnp.float32).astype(jnp.bfloat16)
            wbuf[at] = wbuf[at] * m

    def gather_a():
        def a_step(d, _):
            ga.line(d, True, start)
            return 0

        def a_across(d, _):
            ga.across(d)
            return 0

        lax.fori_loop(1, ga.length, a_step, 0)
        lax.fori_loop(0, ga.length, a_across, 0)

    def compute(slot):
        for bi in range(br):
            k = slot * br + bi
            dev = k // ka
            lanes = pl.ds(pl.multiple_of(lax.rem(k, ka) * tile, tile), tile)
            block = bbuf[slot, bi * tile : (bi + 1) * tile, :]
            for i in range(tr):
                rows = slice(i * tile, (i + 1) * tile)
                acc[rows, :] += jnp.dot(
                    abuf[dev, rows, lanes], block, preferred_element_type=jnp.float32
                )

    half = gb.length

    def step(d, _):
        gb.line(d, True, start)

        @pl.when(d == 1)
        def _():
            gb.divert(0, True, start)
            gather_a()

        gb.divert(d, True, start)

        def near(j, _):
            place = gb.place + jnp.where(j == 0, 0, jnp.where(j == 1, -d, d))
            there = jnp.logical_and(place >= 0, place < half)
            there = jnp.logical_and(there, jnp.logical_or(j > 0, d == 1))
            there = jnp.logical_and(there, jnp.logical_or(j == 0, d < half))

            @pl.when(there)
            def _():
                compute(2 * place + gb.side)
            return 0

        lax.fori_loop(0, 3, near, 0)

        @pl.when(d == half)
        def _():
            masks(True, lambda c: c.wait_recv())

        gb.across(d - 1)

        def far(j, _):
            place = gb.place + jnp.where(j == 0, 1 - d, d - 1)
            there = jnp.logical_and(place >= 0, place < half)
            there = jnp.logical_and(there, jnp.logical_or(j == 0, d > 1))

            @pl.when(there)
            def _():
                compute(2 * place + 1 - gb.side)
            return 0

        lax.fori_loop(0, 2, far, 0)
        return 0

    lax.fori_loop(1, half + 1, step, 0)

    there = {}
    links = [[jnp.zeros((1, 128), jnp.int32) for _ in range(br)] for _ in range(tr)]
    for k in range(ka * n_col):
        for i in range(tr):
            at = i * ka + k % ka
            links[i][k % br] += amask[k // ka][:, at : at + 1] * bmask[k // br]
    for i in range(tr):
        for j in range(tc):
            link = sum(links[i][bi][:, bi * tc + j : bi * tc + j + 1] for bi in range(br))
            there[i, j] = jnp.where(link > 0, wp_ref[i : i + 1, j : j + 1], 0).astype(jnp.float32)
    count = sum(there.values())

    weighted = acc[...] * wbuf[...].astype(jnp.float32)
    obuf[...] = weighted.astype(jnp.bfloat16)
    part = jnp.sum(weighted, axis=0, keepdims=True)
    local_sum = jnp.sum(part, axis=1, keepdims=True)
    ex[me] = jnp.where(lane == 0, local_sum, jnp.where(lane == 1, count, 0.0))

    def ex_start(o, _):
        other = jnp.where(me < everyone // 2, everyone - 1 - o, o)

        @pl.when(other != me)
        def _():
            pltpu.make_async_remote_copy(
                src_ref=ex.at[me], dst_ref=ex.at[me],
                send_sem=ex_send.at[0], recv_sem=ex_recv.at[0],
                device_id=(other // n_col, lax.rem(other, n_col)), device_id_type=MESH,
            ).start()
        return 0

    rest = ex.at[pl.ds(0, everyone - 1)]
    ex_all = pltpu.make_async_remote_copy(
        src_ref=rest, dst_ref=rest, send_sem=ex_send.at[0], recv_sem=ex_recv.at[0],
        device_id={"col": col + 1 - 2 * ga.side}, device_id_type=MESH,
    )

    lax.fori_loop(0, everyone, ex_start, 0)

    gb.own(wait_send)
    ga.own(wait_send)
    masks(False, wait_send)
    gb.divert(0, False, wait_send)

    def drain_b(d, _):
        gb.line(d, False, wait_send)
        gb.divert(d, False, wait_send)
        return 0

    def drain_a(d, _):
        ga.line(d, False, wait_send)
        return 0

    lax.fori_loop(1, half + 1, drain_b, 0)
    lax.fori_loop(1, ga.length, drain_a, 0)

    ex_all.wait_recv()
    everything = ex[...]
    order = lax.broadcasted_iota(jnp.int32, (everyone, 1, 128), 0)
    sums = jnp.sum(everything, axis=0)
    first = jnp.sum(jnp.where(order < me, everything, 0.0), axis=0)
    total_ref[...] = jnp.where(lane == 0, sums, 0.0)
    before = first[:, 1:2]
    for i in range(tr):
        for j in range(tc):
            slot_ref[i : i + 1, j : j + 1] = jnp.where(there[i, j] > 0, before + 1.0, 0.0)
            before = before + there[i, j]
    ex_all.wait_send()


def finish(scale, masked_in, slot_in, total_in, masked_ref, slot_ref, total_ref):
    masked_ref[...] = masked_in[...]
    slot_ref[...] = slot_in[...] - 1.0
    total_ref[...] = total_in[:, 0:1] / scale


def on_device(a_values, a_present, b_values, b_present, w_values, w_present):
    n_row, n_col = lax.axis_size("row"), lax.axis_size("col")
    tr, ka = a_present.shape
    br, tc = b_present.shape
    tile = a_values.shape[0] // tr
    scale = tile * math.sqrt(tr * n_row * tc * n_col)
    everyone = n_row * n_col
    dma = pltpu.SemaphoreType.DMA
    hbm = pl.BlockSpec(memory_space=pl.ANY)
    vmem = pl.BlockSpec(memory_space=pltpu.VMEM)
    masked, slot, total = pl.pallas_call(
        functools.partial(kernel, n_row, n_col, tr, ka, br, tc, tile),
        out_shape=(
            jax.ShapeDtypeStruct(w_values.shape, jnp.bfloat16),
            jax.ShapeDtypeStruct((tr, tc), jnp.float32),
            jax.ShapeDtypeStruct((1, 128), jnp.float32),
        ),
        in_specs=[hbm] * 6,
        out_specs=(vmem, vmem, vmem),
        scratch_shapes=[
            pltpu.VMEM((n_col, *a_values.shape), jnp.bfloat16),
            pltpu.VMEM((n_row, *b_values.shape), jnp.bfloat16),
            pltpu.VMEM(w_values.shape, jnp.bfloat16),
            pltpu.VMEM(w_values.shape, jnp.float32),
            pltpu.VMEM(a_present.shape, jnp.int32),
            pltpu.VMEM(b_present.shape, jnp.int32),
            pltpu.VMEM(w_present.shape, jnp.int32),
            pltpu.VMEM((n_col, 1, 128), jnp.int32),
            pltpu.VMEM((n_row, 1, 128), jnp.int32),
            pltpu.VMEM((everyone, 1, 128), jnp.float32),
            dma((6,)),
            dma((3, n_col, A_PIECES)),
            dma((n_col, A_PIECES)),
            dma((3, n_row, PIECES)),
            dma((n_row, PIECES)),
            dma((n_col,)),
            dma((n_col,)),
            dma((n_row,)),
            dma((n_row,)),
            dma((1,)),
            dma((1,)),
            pltpu.SemaphoreType.REGULAR((6,)),
        ],
        compiler_params=pltpu.CompilerParams(
            collective_id=0, has_side_effects=True, vmem_limit_bytes=56 * 1024 * 1024
        ),
    )(a_values, b_values, w_values, a_present, b_present, w_present)
    masked, slot, total = pl.pallas_call(
        functools.partial(finish, scale),
        out_shape=(
            jax.ShapeDtypeStruct(masked.shape, masked.dtype),
            jax.ShapeDtypeStruct(slot.shape, slot.dtype),
            jax.ShapeDtypeStruct((1, 1), jnp.float32),
        ),
        in_specs=[vmem] * 3,
        out_specs=(vmem, vmem, vmem),
        compiler_params=pltpu.CompilerParams(vmem_limit_bytes=16 * 1024 * 1024),
    )(masked, slot, total)
    return masked, slot, total.reshape(())


def solution(mesh):
    spec = P("row", "col")
    return jax.shard_map(
        on_device, mesh=mesh, in_specs=(spec,) * 6, out_specs=(spec, spec, P()), check_vma=False
    )
```

```python
import functools
import math

import jax
import jax.numpy as jnp
from jax import lax
from jax.experimental import pallas as pl
from jax.experimental.pallas import tpu as pltpu
from jax.sharding import PartitionSpec as P

MESH = pl.DeviceIdType.MESH
PIECES = 2
A_PIECES = 2


class Gather:
    def __init__(self, axis, n, buf, send_sem, recv_sem, pieces, diverted):
        self.axis, self.buf = axis, buf
        self.send_sem, self.recv_sem = send_sem, recv_sem
        self.me = lax.axis_index(axis)
        self.length = n // 2
        self.place, self.side = self.me // 2, self.me % 2
        self.pieces = pieces
        self.height = buf.shape[1] // pieces
        self.diverted = tuple(range(pieces - pieces // 2, pieces)) if diverted else ()

    def copy(self, way, slot, h):
        target = (self.me + 2, self.me - 2, self.me + 1 - 2 * self.side)[way]
        part = self.buf.at[slot, pl.ds(h * self.height, self.height), :]
        return pltpu.make_async_remote_copy(
            src_ref=part,
            dst_ref=part,
            send_sem=self.send_sem.at[way, slot, h],
            recv_sem=self.recv_sem.at[slot, h],
            device_id={self.axis: target},
            device_id_type=MESH,
        )

    def can_up(self):
        return self.place < self.length - 1

    def can_down(self):
        return self.place > 0

    def when_all(self, *conds):
        return pl.when(functools.reduce(jnp.logical_and, conds))

    def run(self, action, way, slot, h, *conds):
        @self.when_all(*conds)
        def _():
            action(self.copy(way, slot, h))

    def own(self, action):
        for h in range(self.pieces):
            self.run(action, 0, self.me, h, self.can_up())
            self.run(action, 1, self.me, h, self.can_down())
            action(self.copy(2, self.me, h))

    def line(self, d, receive, action):
        last = self.length - 1
        for h in range(self.pieces):
            for way, source, onward, end in (
                (0, self.place - d, self.can_up, 0),
                (1, self.place + d, self.can_down, last),
            ):
                slot = 2 * source + self.side
                there = jnp.logical_and(source >= 0, source <= last)
                if receive:
                    self.run(lambda c: c.wait_recv(), 2, slot, h, there)
                self.run(action, way, slot, h, there, onward())
                if h in self.diverted:
                    self.run(action, 2, slot, h, there, source != end)
                else:
                    self.run(action, 2, slot, h, there)

    def divert(self, d, receive, action):
        last = self.length - 1
        for h in self.diverted:
            for way, source, at, onward in (
                (0, 0, d, self.can_up),
                (1, last, last - d, self.can_down),
            ):
                slot = 2 * source + 1 - self.side
                here = self.place == at
                if receive:
                    self.run(lambda c: c.wait_recv(), 2, slot, h, here)
                self.run(action, way, slot, h, here, onward())

    def across(self, d):
        last = self.length - 1
        for h in range(self.pieces):
            for step, end in ((-1, 0), (1, last)):
                source = self.place + step * d
                slot = 2 * source + 1 - self.side
                there = jnp.logical_and(source >= 0, source <= last)
                if step > 0:
                    there = jnp.logical_and(there, d > 0)
                if h in self.diverted:
                    there = jnp.logical_and(there, jnp.logical_and(source != 0, source != last))
                self.run(lambda c: c.wait_recv(), 2, slot, h, there)


def start(c):
    c.start()


def wait_send(c):
    c.wait_send()


def kernel(
    n_row, n_col, tr, ka, br, tc, tile,
    a_hbm, b_hbm, w_hbm, ap_hbm, bp_hbm, wp_hbm,
    obuf, slot_ref, total_ref,
    abuf, bbuf, wbuf, acc, ap_ref, bp_ref, wp_ref, amask, bmask, ex,
    local_sem, a_send, a_recv, b_send, b_recv, am_send, am_recv, bm_send, bm_recv, ex_send, ex_recv, token,
):
    row, col = lax.axis_index("row"), lax.axis_index("col")
    me = row * n_col + col
    everyone = n_row * n_col
    ga = Gather("col", n_col, abuf, a_send, a_recv, A_PIECES, False)
    gb = Gather("row", n_row, bbuf, b_send, b_recv, PIECES, True)

    def signal(sem, g, shift):
        pl.semaphore_signal(sem, inc=1, device_id={g.axis: g.me + shift}, device_id_type=MESH)

    barrier = pltpu.get_barrier_semaphore()
    greeted = 0
    for g in (gb, ga):
        signal(barrier, g, 1 - 2 * g.side)
        pl.when(g.can_up())(functools.partial(signal, barrier, g, 2))
        pl.when(g.can_down())(functools.partial(signal, barrier, g, -2))
        greeted += 1 + g.can_up().astype(jnp.int32) + g.can_down().astype(jnp.int32)

    pairs = (
        (bp_hbm, bp_ref), (b_hbm, bbuf.at[row]), (ap_hbm, ap_ref),
        (a_hbm, abuf.at[col]), (wp_hbm, wp_ref), (w_hbm, wbuf),
    )
    loads = [pltpu.make_async_copy(x, y, local_sem.at[i]) for i, (x, y) in enumerate(pairs)]
    for load in loads:
        load.start()

    def gated(get, put, present, rows, cols):
        for i in range(rows):
            for j in range(cols):
                m = present[i : i + 1, j : j + 1].astype(jnp.float32).astype(jnp.bfloat16)
                put(i, j, get(i, j) * m)

    def gate_block(buf, slot, present, rows, cols):
        def part(i, j):
            return (slot, slice(i * tile, (i + 1) * tile), slice(j * tile, (j + 1) * tile))

        def put(i, j, v):
            buf[part(i, j)] = v

        gated(lambda i, j: buf[part(i, j)], put, present, rows, cols)

    loads[0].wait()
    loads[1].wait()
    gate_block(bbuf, row, bp_ref, br, tc)
    loads[2].wait()
    loads[3].wait()
    gate_block(abuf, col, ap_ref, tr, ka)
    pl.semaphore_wait(barrier, greeted)
    gb.own(start)
    ga.own(start)

    for i, g in enumerate((ga, gb)):
        pair, up, down = token.at[3 * i], token.at[3 * i + 1], token.at[3 * i + 2]
        signal(pair, g, 1 - 2 * g.side)
        if i == 0:
            lane = lax.broadcasted_iota(jnp.int32, (1, 128), 1)

            def packed(ref, rows, cols):
                v = jnp.zeros((1, 128), jnp.int32)
                for r in range(rows):
                    for c in range(cols):
                        v = jnp.where(lane == r * cols + c, ref[r : r + 1, c : c + 1], v)
                return v

            amask[col] = packed(ap_ref, tr, ka)
            bmask[row] = packed(bp_ref, br, tc)
        pl.semaphore_wait(pair, 1)
        last = g.length - 1
        first_up = jnp.logical_and(g.place == 0, g.can_up())
        first_down = jnp.logical_and(g.place == last, g.can_down())
        pl.when(first_up)(functools.partial(signal, up, g, 2))
        pl.when(first_down)(functools.partial(signal, down, g, -2))
        if i == 0:
            acc[...] = jnp.zeros_like(acc)

        @pl.when(g.can_down())
        def _():
            pl.semaphore_wait(up, 1)
            pl.when(g.can_up())(functools.partial(signal, up, g, 2))

        @pl.when(g.can_up())
        def _():
            pl.semaphore_wait(down, 1)
            pl.when(g.can_down())(functools.partial(signal, down, g, -2))

    mask_sets = (
        ("col", col, amask, am_send, am_recv, n_col),
        ("row", row, bmask, bm_send, bm_recv, n_row),
    )

    def masks(arriving, action):
        for axis, mine, buf, send, recv, n in mask_sets:
            def one(o, _):
                other = lax.rem(mine + o, n)
                slot = other if arriving else mine
                action(pltpu.make_async_remote_copy(
                    src_ref=buf.at[slot], dst_ref=buf.at[slot],
                    send_sem=send.at[other], recv_sem=recv.at[slot],
                    device_id={axis: other}, device_id_type=MESH,
                ))
                return 0
            lax.fori_loop(1, n, one, 0)

    masks(False, start)
    loads[4].wait()
    loads[5].wait()
    for i in range(tr):
        for j in range(tc):
            at = (slice(i * tile, (i + 1) * tile), slice(j * tile, (j + 1) * tile))
            m = wp_ref[i : i + 1, j : j + 1].astype(jnp.float32).astype(jnp.bfloat16)
            wbuf[at] = wbuf[at] * m

    def gather_a():
        def a_step(d, _):
            ga.line(d, True, start)
            return 0

        def a_across(d, _):
            ga.across(d)
            return 0

        lax.fori_loop(1, ga.length, a_step, 0)
        lax.fori_loop(0, ga.length, a_across, 0)

    def compute(slot):
        for bi in range(br):
            k = slot * br + bi
            dev = k // ka
            lanes = pl.ds(pl.multiple_of(lax.rem(k, ka) * tile, tile), tile)
            block = bbuf[slot, bi * tile : (bi + 1) * tile, :]
            for i in range(tr):
                rows = slice(i * tile, (i + 1) * tile)
                acc[rows, :] += jnp.dot(
                    abuf[dev, rows, lanes], block, preferred_element_type=jnp.float32
                )

    half = gb.length

    def step(d, _):
        gb.line(d, True, start)

        @pl.when(d == 1)
        def _():
            gb.divert(0, True, start)
            gather_a()

        gb.divert(d, True, start)

        def near(j, _):
            place = gb.place + jnp.where(j == 0, 0, jnp.where(j == 1, -d, d))
            there = jnp.logical_and(place >= 0, place < half)
            there = jnp.logical_and(there, jnp.logical_or(j > 0, d == 1))
            there = jnp.logical_and(there, jnp.logical_or(j == 0, d < half))

            @pl.when(there)
            def _():
                compute(2 * place + gb.side)
            return 0

        lax.fori_loop(0, 3, near, 0)

        @pl.when(d == half)
        def _():
            masks(True, lambda c: c.wait_recv())

        gb.across(d - 1)

        def far(j, _):
            place = gb.place + jnp.where(j == 0, 1 - d, d - 1)
            there = jnp.logical_and(place >= 0, place < half)
            there = jnp.logical_and(there, jnp.logical_or(j == 0, d > 1))

            @pl.when(there)
            def _():
                compute(2 * place + 1 - gb.side)
            return 0

        lax.fori_loop(0, 2, far, 0)
        return 0

    lax.fori_loop(1, half + 1, step, 0)

    there = {}
    links = [[jnp.zeros((1, 128), jnp.int32) for _ in range(br)] for _ in range(tr)]
    for k in range(ka * n_col):
        for i in range(tr):
            at = i * ka + k % ka
            links[i][k % br] += amask[k // ka][:, at : at + 1] * bmask[k // br]
    for i in range(tr):
        for j in range(tc):
            link = sum(links[i][bi][:, bi * tc + j : bi * tc + j + 1] for bi in range(br))
            there[i, j] = jnp.where(link > 0, wp_ref[i : i + 1, j : j + 1], 0).astype(jnp.float32)
    count = sum(there.values())

    weighted = acc[...] * wbuf[...].astype(jnp.float32)
    obuf[...] = weighted.astype(jnp.bfloat16)
    part = jnp.sum(weighted, axis=0, keepdims=True)
    local_sum = jnp.sum(part, axis=1, keepdims=True)
    ex[me] = jnp.where(lane == 0, local_sum, jnp.where(lane == 1, count, 0.0))

    def ex_start(o, _):
        other = jnp.where(me < everyone // 2, everyone - 1 - o, o)

        @pl.when(other != me)
        def _():
            pltpu.make_async_remote_copy(
                src_ref=ex.at[me], dst_ref=ex.at[me],
                send_sem=ex_send.at[0], recv_sem=ex_recv.at[0],
                device_id=(other // n_col, lax.rem(other, n_col)), device_id_type=MESH,
            ).start()
        return 0

    rest = ex.at[pl.ds(0, everyone - 1)]
    ex_all = pltpu.make_async_remote_copy(
        src_ref=rest, dst_ref=rest, send_sem=ex_send.at[0], recv_sem=ex_recv.at[0],
        device_id={"col": col + 1 - 2 * ga.side}, device_id_type=MESH,
    )

    lax.fori_loop(0, everyone, ex_start, 0)

    gb.own(wait_send)
    ga.own(wait_send)
    masks(False, wait_send)
    gb.divert(0, False, wait_send)

    def drain_b(d, _):
        gb.line(d, False, wait_send)
        gb.divert(d, False, wait_send)
        return 0

    def drain_a(d, _):
        ga.line(d, False, wait_send)
        return 0

    lax.fori_loop(1, half + 1, drain_b, 0)
    lax.fori_loop(1, ga.length, drain_a, 0)

    ex_all.wait_recv()
    everything = ex[...]
    order = lax.broadcasted_iota(jnp.int32, (everyone, 1, 128), 0)
    sums = jnp.sum(everything, axis=0)
    first = jnp.sum(jnp.where(order < me, everything, 0.0), axis=0)
    total_ref[...] = jnp.where(lane == 0, sums, 0.0)
    before = first[:, 1:2]
    for i in range(tr):
        for j in range(tc):
            slot_ref[i : i + 1, j : j + 1] = jnp.where(there[i, j] > 0, before + 1.0, 0.0)
            before = before + there[i, j]
    ex_all.wait_send()


def finish(scale, masked_in, slot_in, total_in, masked_ref, slot_ref, total_ref):
    masked_ref[...] = masked_in[...]
    slot_ref[...] = slot_in[...] - 1.0
    total_ref[...] = total_in[:, 0:1] / scale


def on_device(a_values, a_present, b_values, b_present, w_values, w_present):
    n_row, n_col = lax.axis_size("row"), lax.axis_size("col")
    tr, ka = a_present.shape
    br, tc = b_present.shape
    tile = a_values.shape[0] // tr
    scale = tile * math.sqrt(tr * n_row * tc * n_col)
    everyone = n_row * n_col
    dma = pltpu.SemaphoreType.DMA
    hbm = pl.BlockSpec(memory_space=pl.ANY)
    vmem = pl.BlockSpec(memory_space=pltpu.VMEM)
    masked, slot, total = pl.pallas_call(
        functools.partial(kernel, n_row, n_col, tr, ka, br, tc, tile),
        out_shape=(
            pltpu.VMEM(w_values.shape, jnp.bfloat16),
            pltpu.VMEM((tr, tc), jnp.float32),
            pltpu.VMEM((1, 128), jnp.float32),
        ),
        in_specs=[hbm] * 6,
        out_specs=(vmem, vmem, vmem),
        scratch_shapes=[
            pltpu.VMEM((n_col, *a_values.shape), jnp.bfloat16),
            pltpu.VMEM((n_row, *b_values.shape), jnp.bfloat16),
            pltpu.VMEM(w_values.shape, jnp.bfloat16),
            pltpu.VMEM(w_values.shape, jnp.float32),
            pltpu.VMEM(a_present.shape, jnp.int32),
            pltpu.VMEM(b_present.shape, jnp.int32),
            pltpu.VMEM(w_present.shape, jnp.int32),
            pltpu.VMEM((n_col, 1, 128), jnp.int32),
            pltpu.VMEM((n_row, 1, 128), jnp.int32),
            pltpu.VMEM((everyone, 1, 128), jnp.float32),
            dma((6,)),
            dma((3, n_col, A_PIECES)),
            dma((n_col, A_PIECES)),
            dma((3, n_row, PIECES)),
            dma((n_row, PIECES)),
            dma((n_col,)),
            dma((n_col,)),
            dma((n_row,)),
            dma((n_row,)),
            dma((1,)),
            dma((1,)),
            pltpu.SemaphoreType.REGULAR((6,)),
        ],
        compiler_params=pltpu.CompilerParams(
            collective_id=0, has_side_effects=True, vmem_limit_bytes=56 * 1024 * 1024
        ),
    )(a_values, b_values, w_values, a_present, b_present, w_present)
    masked, slot, total = pl.pallas_call(
        functools.partial(finish, scale),
        out_shape=(
            jax.ShapeDtypeStruct(masked.shape, masked.dtype),
            jax.ShapeDtypeStruct(slot.shape, slot.dtype),
            jax.ShapeDtypeStruct((1, 1), jnp.float32),
        ),
        in_specs=[vmem] * 3,
        out_specs=(vmem, vmem, vmem),
        compiler_params=pltpu.CompilerParams(vmem_limit_bytes=16 * 1024 * 1024),
    )(masked, slot, total)
    return masked, slot, total.reshape(())


def solution(mesh):
    spec = P("row", "col")
    return jax.shard_map(
        on_device, mesh=mesh, in_specs=(spec,) * 6, out_specs=(spec, spec, P()), check_vma=False
    )
```
